32 devices in a mesh: tm: 8 (over z, x), gz: 4 (over y, core).
Axes of the slice: x: 2, y: 2, z: 4, core: 2. Of those that a mesh axis runs over, the one named last changes fastest.
Arguments:
- source: float32 [16, 32, 32, 512], P('tm', None, None, 'gz'), may hold values from -8 to 8
- initial_guess: float32 [16, 32, 32, 512], P('tm', None, None, 'gz'), may hold values from -8 to 8
- diffusivity: float32 [32, 32, 512], P(None, None, 'gz'), may hold values from 0.25 to 2.5
Outputs:
- solution: float32 [16, 32, 32, 512], P('tm', None, None, 'gz')
- residual: float32 [16, 32, 32, 512], P('tm', None, None, 'gz')
The draws below stay inside these ranges and needn't reach their ends.
All inputs are finite; a program needn't handle non-finite values.
Results may differ from the reference program's by a relative error of at most 0.00002.
Values sent between devices are 32-bit elements; how exact they have to be, the bound alone decides.
A program may use at most 128 MiB of HBM per device.

```python
import math
import jax
import jax.numpy as jnp

NX = 32
NY = 32
LEVELS = 5
SWEEPS = 2
CSWEEPS = 4
NT = 16
NZ = 512


def level_of(own_key, extent, pieces, smallest, largest):
    gain = 1.0
    for axis_at, shards_of in pieces:
        steps = jax.random.uniform(jax.random.fold_in(jax.random.fold_in(own_key, 6), axis_at), (shards_of,), jnp.float32, smallest / len(pieces), largest / len(pieces))
        gain = gain * jnp.repeat(jnp.exp(steps), extent[axis_at] // shards_of).reshape((-1,) + (1,) * (len(extent) - 1 - axis_at))
    return gain


def noise(key, extent, spread, reach, pieces=(), dtype=jnp.bfloat16):
    entries = jax.random.normal(key, extent, jnp.float32) * spread
    if len(pieces) > 0:
        entries = level_of(key, extent, pieces, -0.22, 0.18) * entries
    return jnp.clip(entries, min=-reach, max=reach).astype(dtype)


def setup_inputs(seed: int = 0) -> dict:
    streams_of = jax.random.split(jax.random.key(seed), 4)
    source = noise(streams_of[0], (NT, NX, NY, NZ), 1.0, 8.0, ((0, 8), (3, 4)), jnp.float32)
    initial_guess = noise(streams_of[1], (NT, NX, NY, NZ), 1.0, 8.0, ((0, 8), (3, 4)), jnp.float32)
    diffusivity = jnp.clip(jnp.exp(math.log(2.5) - 2.3025851 * jax.random.uniform(streams_of[2], (NX, NY, NZ), jnp.float32) ** level_of(streams_of[2], (NX, NY, NZ), ((2, 4),), -0.2, 0.2)), 0.25, 2.5)
    return dict(source=source, initial_guess=initial_guess, diffusivity=diffusivity)


damping = 0.8
base_coef = 8.0


def operate(values, diffusivity, time_coef):
    before = jnp.concatenate([jnp.zeros_like(values[:1]), values[:-1]], axis=0)
    padded = jnp.pad(values, ((0, 0), (1, 1), (1, 1), (1, 1)))
    beside = padded[:, 2:, 1:-1, 1:-1] + padded[:, :-2, 1:-1, 1:-1]
    beside = beside + padded[:, 1:-1, 2:, 1:-1] + padded[:, 1:-1, :-2, 1:-1]
    beside = beside + padded[:, 1:-1, 1:-1, 2:] + padded[:, 1:-1, 1:-1, :-2]
    return time_coef * (values - before) + diffusivity * (6.0 * values - beside)


def smooth(values, target, diffusivity, time_coef, sweep_count):
    scaled = damping / (time_coef + 6.0 * diffusivity)
    for sweep_num in range(sweep_count):
        values = values + scaled * (target - operate(values, diffusivity, time_coef))
    return values


def cycle(level_num, values, target, diffusivity):
    time_coef = base_coef / (2.0 ** level_num)
    if level_num == LEVELS - 1:
        return smooth(values, target, diffusivity, time_coef, CSWEEPS)
    values = smooth(values, target, diffusivity, time_coef, SWEEPS)
    leftover = target - operate(values, diffusivity, time_coef)
    coarse_res = (leftover[0::2] + leftover[1::2]) * 0.5
    correction = cycle(level_num + 1, jnp.zeros_like(coarse_res), coarse_res, diffusivity)
    values = values + jnp.repeat(correction, 2, axis=0)
    return smooth(values, target, diffusivity, time_coef, SWEEPS)


def reference(source, initial_guess, diffusivity):
    solution = cycle(0, initial_guess, source, diffusivity)
    residual = source - operate(solution, diffusivity, base_coef)
    return solution, residual
```

```python
import jax
import jax.numpy as jnp
from jax import lax
from jax.experimental import pallas as pl
from jax.experimental.pallas import tpu as pltpu
from jax.sharding import PartitionSpec as P

LEVELS = 5
damping = 0.8
keep = 1.0 - damping
base_coef = 8.0
F32 = jnp.float32
MESH = pl.DeviceIdType.MESH
LANES = 128
PAD = 8
PX = 4
R = 8
D0 = 8
D1 = 24


def make(mesh, nt, nx, ny, nz):
    ntm, ngz = mesh.shape["tm"], mesh.shape["gz"]
    group = 2 ** (LEVELS - 1) // nt
    groups = ntm // group
    xb = nx // group
    yp = ny + 2 * PAD
    xp = nx + 2 * PX
    rb = LANES // ny
    C = nx // R
    nblk = nx // rb
    times = [0] + [group // 2**l for l in range(LEVELS - 1)]
    hx = [0] + [2] * (LEVELS - 2) + [3]
    xr = [xb + 2 * h for h in hx]
    last = nt - 1

    def kernel(src, guess, dif_hbm, sol, res, *scr):
        scr = list(scr)
        VA, VB, VC, F, DIF, S0, HG, HF, HD = [scr.pop(0) for _ in range(9)]
        rout, es, g1 = HG, HF, HD
        PV = [scr.pop(0) for _ in range(6)]
        PSs, PSr, ZSs, ZSr, DSs, DSr, GSs, GSr, ESs, ESr = [scr.pop(0) for _ in range(10)]
        A = [None] + [[scr.pop(0) for _ in range(3)] for l in range(1, LEVELS)]
        G = [None] + [scr.pop(0) for _ in range(1, LEVELS)]
        E = [None] + [scr.pop(0) for _ in range(1, LEVELS)]
        S = [S0] + [scr.pop(0) for _ in range(1, LEVELS)]
        LP = [None] + [scr.pop(0) for _ in range(1, LEVELS - 1)]
        (load_sem, out_sem, zs_s, zs_r, d_s, d_r, swap_s, swap_r, a_s, a_r, b_s, b_r,
         x_s, x_r, g_s, g_r, t_s, t_r, o_s, o_r) = scr

        tm, gz = lax.axis_index("tm"), lax.axis_index("gz")
        q_t, q_z = lax.rem(tm, 2), lax.rem(gz, 2)
        swapped = q_t != q_z
        stays = q_t == q_z
        I, s = tm - q_t + q_z, gz - q_z + q_t
        grp, i = lax.div(I, group), lax.rem(I, group)
        center = pl.ds(PAD, ny)
        lane = lax.broadcasted_iota(jnp.int32, (ny, nz), 1)
        m0, m1 = lane == 0, lane == nz - 1
        flip = {"tm": tm + 1 - 2 * q_t, "gz": gz + 1 - 2 * q_z}
        mate = {"tm": tm, "gz": gz + 1 - 2 * q_z}

        def holder(ii, ss):
            a, b = lax.rem(ii, 2), lax.rem(ss, 2)
            return {"tm": ii - a + b, "gz": ss - b + a}

        def remote(a, b, ss, rs, where):
            return pltpu.make_async_remote_copy(
                src_ref=a, dst_ref=b, send_sem=ss, recv_sem=rs, device_id=where, device_id_type=MESH)

        sends = []

        def start(cond, c):
            @pl.when(cond)
            def _():
                c.start()
            sends.append((cond, c))

        def recv(cond, c):
            @pl.when(cond)
            def _():
                c.wait_recv()

        def each(count, fn, unroll=1):
            whole = count // unroll

            def steps(k, _):
                for u in range(unroll):
                    fn(k * unroll + u)
                return 0
            lax.fori_loop(0, whole, steps, 0)
            for k in range(whole * unroll, count):
                fn(k)

        home = [pltpu.make_async_copy(guess, HG, load_sem.at[0]),
                pltpu.make_async_copy(src, HF, load_sem.at[1]),
                pltpu.make_async_copy(dif_hbm, HD, load_sem.at[2])]
        for c in (home[2], home[0], home[1]):
            c.start()

        zrow = jnp.zeros((ny, nz), F32)
        zpad = jnp.zeros((PAD, nz), F32)

        def clear_edges(x):
            for v in PV:
                for h in range(2):
                    v[h, x] = zrow
                    v[h, PX + nx + x] = zrow
        each(PX, clear_edges)

        bar = pltpu.get_barrier_semaphore()
        met = [jnp.int32(0)]

        def greet(cond, where):
            @pl.when(cond)
            def _():
                pl.semaphore_signal(bar, inc=1, device_id=where, device_id_type=MESH)
            met[0] = met[0] + jnp.where(cond, 1, 0)

        greet(tm >= 0, mate)
        greet(swapped, flip)
        for d in (-1, 1):
            greet((gz + d >= 0) & (gz + d < ngz), holder(tm, gz + d))
            greet((s + d >= 0) & (s + d < ngz), {"tm": I, "gz": s + d})
            greet((s + d >= 0) & (s + d < ngz), holder(I, s + d))
            greet((I + d >= 0) & (I + d < ntm), holder(I + d, s))
            if groups > 1:
                greet((grp + d >= 0) & (grp + d < groups), holder(I + d * group, s))
        for j in range(1, group):
            greet(tm >= 0, holder(grp * group + lax.rem(i + j, group), s))
        pl.semaphore_wait(bar, met[0])

        moves = []
        for j in range(C):
            rows = pl.ds(R * j, R)
            there = pl.ds(PX + R * j, R)
            for k, (h, v) in enumerate(((guess.at[:, rows], VA.at[:, 0, there, center]),
                                        (src.at[:, rows], F.at[:, 0, there]))):
                n = 2 * j + k
                far = remote(h, v, swap_s.at[n], swap_r.at[n], flip)
                near = pltpu.make_async_copy(h, v, load_sem.at[3 + n])
                start(swapped, far)

                @pl.when(stays)
                def _(near=near):
                    near.start()
                moves.append((far, near))
        dif_own = pltpu.make_async_copy(dif_hbm, DIF.at[0, pl.ds(PX, nx)], load_sem.at[3 + 2 * C])
        dif_far = remote(dif_hbm, DIF.at[0, pl.ds(PX, nx)], swap_s.at[2 * C], swap_r.at[2 * C], mate)
        start(stays, dif_far)

        @pl.when(stays)
        def _():
            dif_own.start()

        def moved(n):
            far, near = moves[n]
            recv(swapped, far)

            @pl.when(stays)
            def _():
                near.wait()

        def clear_v(x):
            for v in (VA, VB, VC):
                for t in range(nt):
                    for h in range(2):
                        v[t, h, x, pl.ds(0, PAD), :] = zpad
                        v[t, h, x, pl.ds(PAD + ny, PAD), :] = zpad
        each(xp, clear_v)

        def clear_x(x):
            for xx in (x, PX + nx + x):
                for h in range(2):
                    for t in range(nt):
                        for v in (VA, VB, VC):
                            v[t, h, xx, center, :] = zrow
                        F[t, h, xx] = zrow
                    DIF[h, xx] = zrow
        each(PX, clear_x)

        @pl.when(I == 0)
        def _():
            def clear_p(x):
                for v in PV:
                    for h in range(2):
                        v[h, PX + x] = zrow
            each(nx, clear_p)
        for l in range(1, LEVELS):
            def clear_a(t, l=l):
                for h in range(2):
                    for a in A[l]:
                        for x in range(xr[l]):
                            a[t + 1, h, x, pl.ds(0, PAD), :] = zpad
                            a[t + 1, h, x, pl.ds(PAD + ny, PAD), :] = zpad
                    for x in range(hx[l]):
                        for xx in (x, hx[l] + xb + x):
                            G[l][t, h, xx] = zrow
                            A[l][1][t + 1, h, xx, center, :] = zrow
            each(times[l], clear_a)

            @pl.when(grp == 0)
            def _(l=l):
                def clear_b(x):
                    for h in range(2):
                        for a in A[l]:
                            a[0, h, x, center, :] = zrow
                each(xr[l], clear_b)

        def pack(block, depth):
            tr = block.reshape(rb * ny, nz).T
            return tr[:depth], tr[nz - depth:]

        def unpack(lo, hi, depth):
            mid = jnp.zeros((nz - 2 * depth, LANES), F32)
            return jnp.concatenate([lo, mid, hi], axis=0).T.reshape(rb, ny, nz)

        for side, edge in ((0, s == ngz - 1), (1, s == 0)):
            @pl.when(edge)
            def _(side=side):
                for z in (ZSr, DSr, GSr):
                    def clear_z(k, z=z):
                        z[side, k] = jnp.zeros(z.shape[2:], F32)
                    each(z.shape[1], clear_z)

        home[2].wait()

        def pack_d(b):
            lo, hi = pack(HD[pl.ds(b * rb, rb)], D1)
            DSs[0, b] = lo
            DSs[1, b] = hi
        each(nblk, pack_d, 2)
        home[0].wait()
        home[1].wait()

        def pack_h(b):
            for k, h in enumerate((HG, HF)):
                for t in range(nt):
                    lo, hi = pack(h[t, pl.ds(b * rb, rb)], D0)
                    n = (k * nt + t) * nblk + b
                    ZSs[0, n] = lo
                    ZSs[1, n] = hi
        each(nblk, pack_h)

        def z_pair(side, a, b, n, home_side):
            d = -1 if side == 0 else 1
            to = holder(tm, gz + d) if home_side else holder(I, s + d)
            c = remote(a.at[side], b.at[side], zs_s.at[n], zs_r.at[n], to)
            base = gz if home_side else s
            can_send = (base + d >= 0) & (base + d < ngz)
            can_recv = (s - d >= 0) & (s - d < ngz)
            return can_send, can_recv, c

        zc = [z_pair(side, a, b, 2 * k + side, True) for k, (a, b) in enumerate(((DSs, DSr), (ZSs, ZSr))) for side in range(2)]
        for cs, cr, c in zc:
            start(cs, c)

        @pl.when(stays)
        def _():
            dif_own.wait()
        recv(swapped, dif_far)
        for cs, cr, c in zc[:2]:
            recv(cr, c)

        def unpack_d(b):
            DIF[1, pl.ds(PX + b * rb, rb)] = unpack(DSr[0, b], DSr[1, b], D1)
        each(nblk, unpack_d, 2)

        def scales(x):
            for h in range(2):
                S0[h, x] = damping / (base_coef + 6.0 * DIF[h, x])
        each(xp, scales)
        row0 = [i * xb + PX - h for h in hx]
        for l in range(1, LEVELS):
            def scales_l(x, l=l):
                for h in range(2):
                    S[l][h, x] = damping / (base_coef / 2.0**l + 6.0 * DIF[h, row0[l] + x])
            each(xr[l], scales_l)
        for cs, cr, c in zc[2:]:
            recv(cr, c)

        def unpack_h(b):
            for t in range(nt):
                VA[t, 1, pl.ds(PX + b * rb, rb), center, :] = unpack(ZSr[0, t * nblk + b], ZSr[1, t * nblk + b], D0)
                F[t, 1, pl.ds(PX + b * rb, rb)] = unpack(ZSr[0, (nt + t) * nblk + b], ZSr[1, (nt + t) * nblk + b], D0)
        each(nblk, unpack_h)

        def gather(v, t, x, parts):
            c = [v[t, h, x, center, :] for h in range(2)]
            up = [pltpu.roll(a, 1, 1) for a in c]
            dn = [pltpu.roll(a, nz - 1, 1) for a in c]
            nb = []
            for h in range(parts):
                a = v[t, h, x + 1, center, :] + v[t, h, x - 1, center, :]
                a = a + (v[t, h, x, pl.ds(PAD + 1, ny), :] + v[t, h, x, pl.ds(PAD - 1, ny), :])
                nb.append(a + (jnp.where(m0, up[1 - h], up[h]) + jnp.where(m1, dn[1 - h], dn[h])))
            return c, nb

        def relax(v, w, t, pv, lo, n):
            def fn(k):
                x = PX + lo + k
                c, nb = gather(v, t, x, 2)
                for h in range(2):
                    b = pv[h, x] if t == 0 else v[t - 1, h, x, center, :]
                    w[t, h, x, center, :] = keep * c[h] + S0[h, x] * ((F[t, h, x] + base_coef * b) + DIF[h, x] * nb[h])
            each(n, fn, 2)

        def residual(v, pv, lo, n, put):
            def fn(k):
                x = PX + lo + k
                d = DIF[0, x]
                rs = []
                b = pv[0, x]
                for t in range(nt):
                    c, nb = gather(v, t, x, 1)
                    rs.append((F[t, 0, x] + base_coef * b) + d * nb[0] - (base_coef + 6.0 * d) * c[0])
                    b = c[0]
                put(lo + k, rs)
            each(n, fn, 2)

        def span(j, off):
            lo = R * j - off
            return lo, (R if j < C - 1 or off == 0 else R + rb)

        def d_copies(n, v, j, off):
            lo, m = span(j, off)
            rows = pl.ds(PX + lo, m)
            k = n * C + j
            bl = pl.ds(j * (R // rb), m // rb)
            own = remote(v.at[last, 0, rows, center], PV[n].at[0, rows], d_s.at[0, k], d_r.at[0, k], holder(I + 1, s))
            halo = remote(PSs.at[n, bl], PSr.at[n, bl], d_s.at[1, k], d_r.at[1, k], holder(I + 1, s))
            return own, halo

        def d_send(n, v, j, off):
            lo, m = span(j, off)

            def fn(b):
                lo8, hi8 = pack(v[last, 1, pl.ds(PX + lo + b * rb, rb), center, :], D0)
                PSs[n, j * (R // rb) + b, pl.ds(0, D0)] = lo8
                PSs[n, j * (R // rb) + b, pl.ds(D0, D0)] = hi8
            each(m // rb, fn, 2)
            own, halo = d_copies(n, v, j, off)
            start(I < ntm - 1, own)
            start(I < ntm - 1, halo)

        def d_recv(n, v, j, off):
            lo, m = span(j, off)
            own, halo = d_copies(n, v, j, off)

            @pl.when(I > 0)
            def _():
                own.wait_recv()
                halo.wait_recv()

                def fn(b):
                    k = j * (R // rb) + b
                    PV[n][1, pl.ds(PX + lo + b * rb, rb)] = unpack(PSr[n, k, pl.ds(0, D0)], PSr[n, k, pl.ds(D0, D0)], D0)
                each(m // rb, fn, 2)

        def phase(v, w, u, n, arrive, put, after2, after_r):
            for j in range(C + 2):
                if j < C:
                    arrive(j)
                    d_send(n, v, j, 0)
                    for t in range(nt - 1, 0, -1):
                        relax(v, w, t, None, *span(j, 1))
                    d_send(n + 1, w, j, 1)
                if 1 <= j <= C:
                    d_recv(n, v, j - 1, 0)
                    relax(v, w, 0, PV[n], *span(j - 1, 1))
                    for t in range(nt - 1, 0, -1):
                        relax(w, u, t, None, *span(j - 1, 2))
                    d_send(n + 2, u, j - 1, 2)
                    d_recv(n + 1, w, j - 1, 1)
                    relax(w, u, 0, PV[n + 1], *span(j - 1, 2))
                    after2(j - 1)
                if j >= 2:
                    d_recv(n + 2, u, j - 2, 2)
                    lo = max(R * (j - 2) - 3, 0)
                    hi = R * (j - 1) - 3 if j - 2 < C - 1 else nx
                    residual(u, PV[n + 2], lo, hi - lo, put)
                    after_r(j - 2, lo, hi)

        def a2a(o, at):
            return remote(g1.at[pl.ds(o * xb, xb)], G[1].at[at, 0, pl.ds(hx[1], xb)], a_s.at[o], a_r.at[at], holder(grp * group + o, s))

        def arrive_in(j):
            moved(2 * j)
            moved(2 * j + 1)

        def put_g(x, rs):
            g1[x] = (rs[0] + rs[1]) * 0.5

        done = [0]

        def spread(j, lo, hi):
            while done[0] < group and (done[0] + 1) * xb <= hi:
                o = done[0]
                start(i != o, a2a(o, i))

                @pl.when(i == o)
                def _(o=o):
                    for x in range(xb):
                        G[1][i, 0, hx[1] + x] = g1[o * xb + x]
                done[0] += 1

        phase(VA, VB, VC, 0, arrive_in, put_g, lambda j: None, spread)

        for o in range(group):
            recv(i != o, a2a(o, o))
        turn = {"x": 0, "t": 0}

        bpr = xb // rb

        def g_strip(k):
            t, b = lax.div(k, bpr), lax.rem(k, bpr)
            lo, hi = pack(G[1][t, 0, pl.ds(hx[1] + b * rb, rb)], D1)
            GSs[0, k] = lo
            GSs[1, k] = hi
        each(times[1] * bpr, g_strip, 2)
        gc = [z_pair(side, GSs, GSr, 4 + side, False) for side in range(2)]
        for cs, cr, c in gc:
            start(cs, c)
        for cs, cr, c in gc:
            recv(cr, c)

        def g_unstrip(k):
            t, b = lax.div(k, bpr), lax.rem(k, bpr)
            G[1][t, 1, pl.ds(hx[1] + b * rb, rb)] = unpack(GSr[0, k], GSr[1, k], D1)
        each(times[1] * bpr, g_unstrip, 2)

        def x_halo(at, H, depth):
            n = turn["x"]
            turn["x"] += 1
            lo = remote(at(pl.ds(H, depth)), at(pl.ds(H + xb, depth)), x_s.at[0, n], x_r.at[0, n], holder(I - 1, s))
            hi = remote(at(pl.ds(H + xb - depth, depth)), at(pl.ds(H - depth, depth)), x_s.at[1, n], x_r.at[1, n],
                        holder(I + 1, s))
            start(i > 0, lo)
            start(i < group - 1, hi)
            recv(i > 0, hi)
            recv(i < group - 1, lo)

        def t_halo(l, ver, depth, lifted=False):
            if groups == 1:
                return
            lo, n = hx[l] - depth, xb + 2 * depth
            k = turn["t"]
            turn["t"] += 1
            a, T = A[l][ver], times[l]
            rows = pl.ds(lo, n)
            to = LP[l].at[:, rows] if lifted else a.at[0, :, rows, center]
            c = remote(a.at[T, :, rows, center], to, t_s.at[k], t_r.at[k], holder(I + group, s))
            start(grp < groups - 1, c)
            recv(grp > 0, c)
            if lifted:
                @pl.when(grp > 0)
                def _():
                    for x in range(lo, lo + n):
                        for h in range(2):
                            a[0, h, x, center, :] = LP[l][h, x]

        def coarse_rows(l, lo, n, fn, steps=None):
            def step(t):
                for k in range(n):
                    fn(t, lo + k)
            each(times[l] if steps is None else steps, step)

        def first(l, depth):
            lo, n = hx[l] - depth, xb + 2 * depth

            def fn(t, x):
                for h in range(2):
                    A[l][0][t + 1, h, x, center, :] = S[l][h, x] * G[l][t, h, x]
            coarse_rows(l, lo, n, fn)
            t_halo(l, 0, depth)

        def relaxed(l, ver, depth, put):
            a = A[l][ver]
            coef = base_coef / 2.0**l

            def fn(t, x):
                c, nb = gather(a, t + 1, x, 2)
                for h in range(2):
                    b = a[t, h, x, center, :]
                    put(t, h, x, keep * c[h] + S[l][h, x] * ((G[l][t, h, x] + coef * b) + DIF[h, row0[l] + x] * nb[h]))
            coarse_rows(l, hx[l] - depth, xb + 2 * depth, fn)

        def into(l, ver):
            def put(t, h, x, val):
                A[l][ver][t + 1, h, x, center, :] = val
            return put

        def finish(l):
            def put(t, h, x, val):
                E[l][t, h, x - hx[l]] = val
            return put

        def coarse(l):
            H = hx[l]
            x_halo(lambda rows: G[l].at[:, :, rows], H, H)
            first(l, H)
            if l == LEVELS - 1:
                relaxed(l, 0, 2, into(l, 1))
                t_halo(l, 1, 2)
                relaxed(l, 1, 1, into(l, 2))
                t_halo(l, 2, 1)
                relaxed(l, 2, 0, finish(l))
                return
            relaxed(l, 0, 1, into(l, 1))
            t_halo(l, 1, 1)
            coef = base_coef / 2.0**l

            def down(t, x):
                parts = []
                d = [DIF[h, row0[l] + x] for h in range(2)]
                for k in range(2):
                    c, nb = gather(A[l][1], 2 * t + k + 1, x, 2)
                    parts.append([(G[l][2 * t + k, h, x] + coef * A[l][1][2 * t + k, h, x, center, :]) + d[h] * nb[h]
                                  - (coef + 6.0 * d[h]) * c[h] for h in range(2)])
                for h in range(2):
                    G[l + 1][t, h, x - H + hx[l + 1]] = (parts[0][h] + parts[1][h]) * 0.5
            coarse_rows(l, H, xb, down, times[l + 1])
            coarse(l + 1)

            def lift(t, x):
                for h in range(2):
                    A[l][1][t + 1, h, x, center, :] = A[l][1][t + 1, h, x, center, :] + E[l + 1][lax.div(t, 2), h, x - H]
            coarse_rows(l, H, xb, lift)
            T = times[l]
            x_halo(lambda rows: A[l][1].at[pl.ds(1, T), :, rows, center], H, 2)
            t_halo(l, 1, 2, True)
            relaxed(l, 1, 1, into(l, 2))
            t_halo(l, 2, 1)
            relaxed(l, 2, 0, finish(l))

        coarse(1)

        def e_strip(k):
            t, b = lax.div(k, bpr), lax.rem(k, bpr)
            lo, hi = pack(E[1][t, 1, pl.ds(b * rb, rb)], D0)
            ESs[k, pl.ds(0, D0)] = lo
            ESs[k, pl.ds(D0, D0)] = hi
        each(times[1] * bpr, e_strip, 2)

        def back(other, at, j):
            to = holder(grp * group + other, s)
            return (remote(E[1].at[other, 0], es.at[0, pl.ds(at * xb, xb)], b_s.at[0, j], b_r.at[0, j], to),
                    remote(ESs.at[pl.ds(other * bpr, bpr)], ESr.at[pl.ds(at * bpr, bpr)], b_s.at[1, j], b_r.at[1, j], to))

        for j in range(1, group):
            for c in back(lax.rem(i + j, group), i, j):
                start(tm >= 0, c)
        for x in range(xb):
            es[0, i * xb + x] = E[1][i, 0, x]
        for b in range(bpr):
            ESr[i * bpr + b] = ESs[i * bpr + b]
        for j in range(1, group):
            for c in back(lax.rem(i + j, group), lax.rem(i + group - j, group), j):
                c.wait_recv()

        def arrive_up(j):
            def fn(b):
                k = j * (R // rb) + b
                es[1, pl.ds(k * rb, rb)] = unpack(ESr[k, pl.ds(0, D0)], ESr[k, pl.ds(D0, D0)], D0)
            each(R // rb, fn, 2)

            def lift(k):
                x = R * j + k
                for h in range(2):
                    e = es[h, x]
                    for t in range(nt):
                        VC[t, h, PX + x, center, :] = VC[t, h, PX + x, center, :] + e
            each(R, lift, 2)

        outs = []

        def emit(a, b, n):
            far = remote(a, b, o_s.at[n], o_r.at[n], flip)
            near = pltpu.make_async_copy(a, b, out_sem.at[n])
            start(swapped, far)

            @pl.when(stays)
            def _():
                near.start()
            outs.append((far, near))

        def emit_sol(j):
            lo, m = span(j, 2)
            hi = nx if j == C - 1 else lo + m
            lo = max(lo, 0)
            emit(VB.at[:, 0, pl.ds(PX + lo, hi - lo), center], sol.at[:, pl.ds(lo, hi - lo)], j)

        def put_r(x, rs):
            for t in range(nt):
                rout[t, x] = rs[t]

        def emit_res(j, lo, hi):
            emit(rout.at[:, pl.ds(lo, hi - lo)], res.at[:, pl.ds(lo, hi - lo)], C + j)

        for cond, c in sends:
            @pl.when(cond)
            def _(c=c):
                c.wait_send()
        sends.clear()
        phase(VC, VA, VB, 3, arrive_up, put_r, emit_sol, emit_res)
        for far, near in outs:
            recv(swapped, far)

            @pl.when(stays)
            def _(near=near):
                near.wait()
        for cond, c in sends:
            @pl.when(cond)
            def _(c=c):
                c.wait_send()

    dma = pltpu.SemaphoreType.DMA
    vm = lambda *shape: pltpu.VMEM(shape, F32)
    bpr = xb // rb
    n_t = 4 * (LEVELS - 2) + 3
    n_x = 2 * (LEVELS - 2) + 1
    scratch = [vm(nt, 2, xp, yp, nz)] * 3
    scratch += [vm(nt, 2, xp, ny, nz), vm(2, xp, ny, nz), vm(2, xp, ny, nz)]
    scratch += [vm(nt, nx, ny, nz), vm(nt, nx, ny, nz), vm(nx, ny, nz)]
    scratch += [vm(2, xp, ny, nz)] * 6
    scratch += [vm(6, nblk + 1, 2 * D0, LANES)] * 2
    scratch += [vm(2, 2 * nt * nblk, D0, LANES)] * 2
    scratch += [vm(2, nblk, D1, LANES)] * 2
    scratch += [vm(2, times[1] * bpr, D1, LANES)] * 2
    scratch += [vm(times[1] * bpr, 2 * D0, LANES), vm(nblk, 2 * D0, LANES)]
    for l in range(1, LEVELS):
        scratch += [vm(times[l] + 1, 2, xr[l], yp, nz)] * 3
    scratch += [vm(times[l], 2, xr[l], ny, nz) for l in range(1, LEVELS)]
    scratch += [vm(times[l], 2, xb, ny, nz) for l in range(1, LEVELS)]
    scratch += [vm(2, xr[l], ny, nz) for l in range(1, LEVELS)]
    scratch += [vm(2, xr[l], ny, nz) for l in range(1, LEVELS - 1)]
    scratch += [dma((3 + 2 * C + 1,)), dma((2 * C,)), dma((6,)), dma((6,)), dma((2, 6 * C)), dma((2, 6 * C)),
                dma((2 * C + 1,)), dma((2 * C + 1,)), dma((group,)), dma((group,)), dma((2, group)), dma((2, group)),
                dma((2, n_x)), dma((2, n_x)), dma((1,)), dma((1,)), dma((n_t,)), dma((n_t,)), dma((2 * C,)), dma((2 * C,))]
    shape = jax.ShapeDtypeStruct((nt, nx, ny, nz), F32)
    anyspec = pl.BlockSpec(memory_space=pl.ANY)
    return pl.pallas_call(
        kernel,
        out_shape=(shape, shape),
        in_specs=[anyspec] * 3,
        out_specs=(anyspec, anyspec),
        scratch_shapes=scratch,
        compiler_params=pltpu.CompilerParams(collective_id=0, has_side_effects=True, vmem_limit_bytes=63 << 20),
    )


def solution(mesh):
    def body(source, initial_guess, diffusivity):
        return make(mesh, *source.shape)(source, initial_guess, diffusivity)

    placed = (P("tm", None, None, "gz"), P("tm", None, None, "gz"), P(None, None, "gz"))
    return jax.shard_map(
        body,
        mesh=mesh,
        in_specs=placed,
        out_specs=(P("tm", None, None, "gz"), P("tm", None, None, "gz")),
        check_vma=False,
    )
```

```python
import jax
import jax.numpy as jnp
from jax import lax
from jax.experimental import pallas as pl
from jax.experimental.pallas import tpu as pltpu
from jax.sharding import PartitionSpec as P

LEVELS = 5
damping = 0.8
keep = 1.0 - damping
base_coef = 8.0
F32 = jnp.float32
MESH = pl.DeviceIdType.MESH
LANES = 128
PAD = 8
PX = 4
D0 = 8
D1 = 16
NP = 10


def make(mesh, nt, nx, ny, nz):
    ntm, ngz = mesh.shape["tm"], mesh.shape["gz"]
    group = 2 ** (LEVELS - 1) // nt
    groups = ntm // group
    xb = nx // group
    yp = ny + 2 * PAD
    xp = nx + 2 * PX
    rb = LANES // ny
    q = nx // 8
    cuts = {"down": [0, 2 * q, 4 * q, 6 * q, nx], "up": [0, 2 * q, 4 * q, 6 * q, nx]}
    C = len(cuts["down"]) - 1
    nblk = nx // rb
    times = [0] + [group // 2**l for l in range(LEVELS - 1)]
    hx = [0] + [2] * (LEVELS - 2) + [3]
    xr = [xb + 2 * h for h in hx]
    last = nt - 1

    def kernel(src, guess, dif_hbm, sol, res, *scr):
        scr = list(scr)
        VA, VB, VC, WA, WB, F, GL, DIF, S0, S1, HG, HF, HD, RB = [scr.pop(0) for _ in range(14)]
        rout, es, g1 = HG, HF, HD
        PV = [scr.pop(0) for _ in range(NP)]
        PSs, PSr, ZGs, ZGr, ZFs, ZFr, DSs, DSr, GSs, GSr, ESs, ESr = [scr.pop(0) for _ in range(12)]
        A = [None] * 2 + [[scr.pop(0) for _ in range(3)] for l in range(2, LEVELS)]
        G = [None] * 2 + [scr.pop(0) for _ in range(2, LEVELS)]
        E = [None] * 2 + [scr.pop(0) for _ in range(2, LEVELS)]
        S = [S0, S1] + [scr.pop(0) for _ in range(2, LEVELS)]
        LP = [None] * 2 + [scr.pop(0) for _ in range(2, LEVELS - 1)]
        (load_sem, out_sem, zs_s, zs_r, d_s, d_r, swap_s, swap_r, a_s, a_r, b_s, b_r,
         x_s, x_r, g_s, g_r, t_s, t_r, o_s, o_r, p_s, p_r, f_s, f_r) = scr

        tm, gz = lax.axis_index("tm"), lax.axis_index("gz")
        q_t, q_z = lax.rem(tm, 2), lax.rem(gz, 2)
        swapped = q_t != q_z
        stays = q_t == q_z
        I, s = tm - q_t + q_z, gz - q_z + q_t
        grp, i = lax.div(I, group), lax.rem(I, group)
        center = pl.ds(PAD, ny)
        lane = lax.broadcasted_iota(jnp.int32, (ny, nz), 1)
        m0, m1 = lane == 0, lane == nz - 1
        flip = {"tm": tm + 1 - 2 * q_t, "gz": gz + 1 - 2 * q_z}
        mate = {"tm": tm, "gz": gz + 1 - 2 * q_z}
        par, z = q_z, lax.div(i, 2)

        def holder(ii, ss):
            a, b = lax.rem(ii, 2), lax.rem(ss, 2)
            return {"tm": ii - a + b, "gz": ss - b + a}

        def remote(a, b, ss, rs, where):
            return pltpu.make_async_remote_copy(
                src_ref=a, dst_ref=b, send_sem=ss, recv_sem=rs, device_id=where, device_id_type=MESH)

        sends = []

        def start(cond, c):
            @pl.when(cond)
            def _():
                c.start()
            sends.append((cond, c))

        def recv(cond, c):
            @pl.when(cond)
            def _():
                c.wait_recv()

        def each(count, fn, unroll=1):
            whole = count // unroll

            def steps(k, _):
                for u in range(unroll):
                    fn(k * unroll + u)
                return 0
            lax.fori_loop(0, whole, steps, 0)
            for k in range(whole * unroll, count):
                fn(k)

        home = [pltpu.make_async_copy(guess, HG, load_sem.at[0]),
                pltpu.make_async_copy(src, HF, load_sem.at[1]),
                pltpu.make_async_copy(dif_hbm, HD, load_sem.at[2])]
        for c in (home[2], home[0], home[1]):
            c.start()

        zrow = jnp.zeros((ny, nz), F32)
        zpad = jnp.zeros((PAD, nz), F32)

        def clear_edges(x):
            for v in PV:
                for h in range(2):
                    v[h, x] = zrow
                    v[h, PX + nx + x] = zrow
        each(PX, clear_edges)

        bar = pltpu.get_barrier_semaphore()
        met = [jnp.int32(0)]

        def greet(cond, where):
            @pl.when(cond)
            def _():
                pl.semaphore_signal(bar, inc=1, device_id=where, device_id_type=MESH)
            met[0] = met[0] + jnp.where(cond, 1, 0)

        greet(tm >= 0, mate)
        greet(swapped, flip)
        for d in (-1, 1):
            greet((gz + d >= 0) & (gz + d < ngz), holder(tm, gz + d))
            greet((s + d >= 0) & (s + d < ngz), {"tm": I, "gz": s + d})
            greet((s + d >= 0) & (s + d < ngz), holder(I, s + d))
            greet((I + d >= 0) & (I + d < ntm), holder(I + d, s))
            if groups > 1:
                greet((grp + d >= 0) & (grp + d < groups), holder(I + d * group, s))
        for j in range(1, group):
            greet(tm >= 0, holder(grp * group + lax.rem(i + j, group), s))
            if j % 2 == 0:
                for d in (-1, 1):
                    greet((s + d >= 0) & (s + d < ngz), holder(grp * group + lax.rem(i + j, group), s + d))
        pl.semaphore_wait(bar, met[0])

        moves = {}
        for k in range(2):
            for j in range(C):
                first, many = cuts["down"][j], cuts["down"][j + 1] - cuts["down"][j]
                rows, there = pl.ds(first, many), pl.ds(PX + first, many)
                h, v = ((guess.at[:, rows], VA.at[:, 0, there, center]) if k == 0 else
                        (src.at[:, rows], F.at[:, 0, there]))
                n = 2 * j + k
                far = remote(h, v, swap_s.at[n], swap_r.at[n], flip)
                near = pltpu.make_async_copy(h, v, load_sem.at[3 + n])
                start(swapped, far)

                @pl.when(stays)
                def _(near=near):
                    near.start()
                moves[n] = (far, near)
        dif_own = pltpu.make_async_copy(dif_hbm, DIF.at[0, pl.ds(PX, nx)], load_sem.at[3 + 2 * C])
        dif_far = remote(dif_hbm, DIF.at[0, pl.ds(PX, nx)], swap_s.at[2 * C], swap_r.at[2 * C], mate)
        start(stays, dif_far)

        @pl.when(stays)
        def _():
            dif_own.start()

        def moved(n):
            far, near = moves[n]
            recv(swapped, far)

            @pl.when(stays)
            def _():
                near.wait()

        def clear_v(x):
            for v in (VA, VB, VC):
                for t in range(nt):
                    for h in range(2):
                        v[t, h, x, pl.ds(0, PAD), :] = zpad
                        v[t, h, x, pl.ds(PAD + ny, PAD), :] = zpad
            for v in (WA, WB):
                for h in range(2):
                    v[0, h, x, pl.ds(0, PAD), :] = zpad
                    v[0, h, x, pl.ds(PAD + ny, PAD), :] = zpad
        each(xp, clear_v)

        def clear_x(x):
            for xx in (x, PX + nx + x):
                for h in range(2):
                    for t in range(nt):
                        for v in (VA, VB, VC):
                            v[t, h, xx, center, :] = zrow
                        F[t, h, xx] = zrow
                    for v in (WA, WB):
                        v[0, h, xx, center, :] = zrow
                    DIF[h, xx] = zrow
                    GL[h, xx] = zrow
        each(PX, clear_x)

        @pl.when(I == 0)
        def _():
            def clear_p(x):
                for v in PV:
                    for h in range(2):
                        v[h, PX + x] = zrow
            each(nx, clear_p)
        for l in range(2, LEVELS):
            def clear_a(t, l=l):
                for h in range(2):
                    for a in A[l]:
                        for x in range(xr[l]):
                            a[t + 1, h, x, pl.ds(0, PAD), :] = zpad
                            a[t + 1, h, x, pl.ds(PAD + ny, PAD), :] = zpad
                    for x in range(hx[l]):
                        for xx in (x, hx[l] + xb + x):
                            G[l][t, h, xx] = zrow
                            A[l][1][t + 1, h, xx, center, :] = zrow
            each(times[l], clear_a)

            @pl.when(grp == 0)
            def _(l=l):
                def clear_b(x):
                    for h in range(2):
                        for a in A[l]:
                            a[0, h, x, center, :] = zrow
                each(xr[l], clear_b)

        def pack(block, depth):
            tr = block.reshape(rb * ny, nz).T
            return tr[:depth], tr[nz - depth:]

        def unpack(lo, hi, depth):
            mid = jnp.zeros((nz - 2 * depth, LANES), F32)
            return jnp.concatenate([lo, mid, hi], axis=0).T.reshape(rb, ny, nz)

        for side, edge in ((0, s == ngz - 1), (1, s == 0)):
            @pl.when(edge)
            def _(side=side):
                for a in (ZGr, ZFr, DSr, GSr):
                    def clear_z(k, a=a):
                        a[side, k] = jnp.zeros(a.shape[2:], F32)
                    each(a.shape[1], clear_z)

        home[2].wait()

        def pack_d(b):
            lo, hi = pack(HD[pl.ds(b * rb, rb)], D1)
            DSs[0, b] = lo
            DSs[1, b] = hi
        each(nblk, pack_d, 2)
        home[0].wait()
        home[1].wait()

        def pack_h(b):
            for h, a, depth in ((HG, ZGs, D1), (HF, ZFs, D0)):
                for t in range(nt):
                    lo, hi = pack(h[t, pl.ds(b * rb, rb)], depth)
                    a[0, t * nblk + b] = lo
                    a[1, t * nblk + b] = hi
        each(nblk, pack_h)

        def z_pair(side, a, b, n, home_side):
            d = -1 if side == 0 else 1
            to = holder(tm, gz + d) if home_side else holder(I, s + d)
            c = remote(a.at[side], b.at[side], zs_s.at[n], zs_r.at[n], to)
            base = gz if home_side else s
            can_send = (base + d >= 0) & (base + d < ngz)
            can_recv = (s - d >= 0) & (s - d < ngz)
            return can_send, can_recv, c

        zc = [z_pair(side, a, b, 2 * k + side, True) for k, (a, b) in enumerate(((DSs, DSr), (ZGs, ZGr), (ZFs, ZFr))) for side in range(2)]
        for cs, cr, c in zc:
            start(cs, c)

        @pl.when(stays)
        def _():
            dif_own.wait()
        recv(swapped, dif_far)
        for cs, cr, c in zc[:2]:
            recv(cr, c)

        def unpack_d(b):
            DIF[1, pl.ds(PX + b * rb, rb)] = unpack(DSr[0, b], DSr[1, b], D1)
        each(nblk, unpack_d, 2)

        def scales(x):
            for h in range(2):
                S0[h, x] = damping / (base_coef + 6.0 * DIF[h, x])
                S1[h, x] = damping / (base_coef / 2.0 + 6.0 * DIF[h, x])
        each(xp, scales)
        row0 = [i * xb + PX - h for h in hx]
        for l in range(2, LEVELS):
            def scales_l(x, l=l):
                for h in range(2):
                    S[l][h, x] = damping / (base_coef / 2.0**l + 6.0 * DIF[h, row0[l] + x])
            each(xr[l], scales_l)
        for cs, cr, c in zc[2:4]:
            recv(cr, c)

        def unpack_g(b):
            for t in range(nt):
                VA[t, 1, pl.ds(PX + b * rb, rb), center, :] = unpack(ZGr[0, t * nblk + b], ZGr[1, t * nblk + b], D1)
        each(nblk, unpack_g, 2)

        def unpack_f(b):
            for t in range(nt):
                F[t, 1, pl.ds(PX + b * rb, rb)] = unpack(ZFr[0, t * nblk + b], ZFr[1, t * nblk + b], D0)

        def gather(v, t, x, parts):
            c = [v[t, h, x, center, :] for h in range(2)]
            up = [pltpu.roll(a, 1, 1) for a in c]
            dn = [pltpu.roll(a, nz - 1, 1) for a in c]
            nb = []
            for h in range(parts):
                a = v[t, h, x + 1, center, :] + v[t, h, x - 1, center, :]
                a = a + (v[t, h, x, pl.ds(PAD + 1, ny), :] + v[t, h, x, pl.ds(PAD - 1, ny), :])
                nb.append(a + (jnp.where(m0, up[1 - h], up[h]) + jnp.where(m1, dn[1 - h], dn[h])))
            return c, nb

        fine = (lambda t, h, x: F[t, h, x], S0, base_coef)
        second = (lambda t, h, x: GL[h, x], S1, base_coef / 2.0)

        def relaxed_row(lev, v, t, pv, x):
            g, sc, coef = lev
            c, nb = gather(v, t, x, 2)
            b = [pv[h, x] if t == 0 else v[t - 1, h, x, center, :] for h in range(2)]
            return [keep * c[h] + sc[h, x] * ((g(t, h, x) + coef * b[h]) + DIF[h, x] * nb[h]) for h in range(2)]

        def relax(lev, v, w, t, pv, lo, n):
            def fn(k):
                x = PX + lo + k
                val = relaxed_row(lev, v, t, pv, x)
                for h in range(2):
                    w[t, h, x, center, :] = val[h]
            each(n, fn, 8)

        def residual(lev, v, steps, pv, lo, n, parts, put):
            g, _, coef = lev

            def fn(k):
                x = PX + lo + k
                d = [DIF[h, x] for h in range(parts)]
                b = [pv[h, x] for h in range(parts)]
                rs = []
                for t in range(steps):
                    c, nb = gather(v, t, x, parts)
                    rs.append([(g(t, h, x) + coef * b[h]) + d[h] * nb[h] - (coef + 6.0 * d[h]) * c[h] for h in range(parts)])
                    b = c
                put(lo + k, rs)
            each(n, fn, 4 if parts * steps > 2 else 8)

        B = list(cuts["down"])

        def span(j, off):
            hi = B[j + 1] - off if j < C - 1 else nx
            if j == 0:
                m = -(-hi // rb) * rb
                return hi - m, m
            return B[j] - off, -(-(hi - B[j] + off) // rb) * rb

        def block0(j):
            return B[j] // rb

        def inside(j, off):
            return max(B[j] - off, 0), (B[j + 1] - off if j < C - 1 else nx)

        def d_copies(n, v, t, j, off):
            lo, m = span(j, off)
            rows = pl.ds(PX + lo, m)
            k = n * C + j
            bl = pl.ds(block0(j), m // rb)
            own = remote(v.at[t, 0, rows, center], PV[n].at[0, rows], d_s.at[0, k], d_r.at[0, k], holder(I + 1, s))
            halo = remote(PSs.at[n, bl], PSr.at[n, bl], d_s.at[1, k], d_r.at[1, k], holder(I + 1, s))
            return own, halo

        def d_send(n, v, t, j, off):
            lo, m = span(j, off)

            def fn(b):
                lo8, hi8 = pack(v[t, 1, pl.ds(PX + lo + b * rb, rb), center, :], D0)
                PSs[n, block0(j) + b, pl.ds(0, D0)] = lo8
                PSs[n, block0(j) + b, pl.ds(D0, D0)] = hi8
            own, halo = d_copies(n, v, t, j, off)
            start(I < ntm - 1, own)
            each(m // rb, fn, 3)
            start(I < ntm - 1, halo)

        def d_recv(n, v, t, j, off):
            lo, m = span(j, off)
            own, halo = d_copies(n, v, t, j, off)

            @pl.when(I > 0)
            def _():
                own.wait_recv()
                halo.wait_recv()

                def fn(b):
                    k = block0(j) + b
                    PV[n][1, pl.ds(PX + lo + b * rb, rb)] = unpack(PSr[n, k, pl.ds(0, D0)], PSr[n, k, pl.ds(D0, D0)], D0)
                each(m // rb, fn, 3)

        before = range(nt - 1, 0, -1)

        def put_g(x, rs):
            for h in range(2):
                g = (rs[0][h] + rs[1][h]) * 0.5
                GL[h, PX + x] = g
                WA[0, h, PX + x, center, :] = S1[h, PX + x] * g

        def put_r1(x, rs):
            g1[x] = rs[0][0]

        bpr = xb // rb
        buddy = holder(I + 1 - 2 * par, s)

        def to_buddy(o):
            rows = pl.ds(o * xb, xb)
            return remote(g1.at[rows], RB.at[rows], p_s.at[o], p_r.at[o], buddy)

        def to_owner(o, at):
            return remote(g1.at[pl.ds(o * xb, xb)], G[2].at[at, 0, pl.ds(hx[2], xb)], a_s.at[o], a_r.at[at],
                          holder(grp * group + o, s))

        def strip_to(side, o, at):
            d = -1 if side == 0 else 1
            return remote(GSs.at[side, pl.ds(o * bpr, bpr)], GSr.at[side, pl.ds(at * bpr, bpr)], g_s.at[side, o],
                          g_r.at[side, at], holder(grp * group + o, s + d))

        ready, sent = [0], [0]

        def offer(hi):
            while ready[0] < group and (ready[0] + 1) * xb <= hi:
                start(par != ready[0] % 2, to_buddy(ready[0]))
                ready[0] += 1

        def spread():
            while sent[0] < ready[0]:
                o = sent[0]
                sent[0] += 1
                mine = par == o % 2
                recv(mine, to_buddy(o))

                @pl.when(mine)
                def _(o=o):
                    def fn(b):
                        rows = pl.ds(o * xb + b * rb, rb)
                        g = (g1[rows] + RB[rows]) * 0.5
                        g1[rows] = g
                        lo, hi = pack(g, D1)
                        GSs[0, o * bpr + b] = lo
                        GSs[1, o * bpr + b] = hi
                    each(bpr, fn)
                start(mine & (i != o), to_owner(o, z))
                start(mine & (s > 0), strip_to(0, o, z))
                start(mine & (s < ngz - 1), strip_to(1, o, z))

                @pl.when(i == o)
                def _(o=o):
                    for x in range(xb):
                        G[2][z, 0, hx[2] + x] = g1[o * xb + x]

        for j in range(C):
            moved(2 * j)
            d_send(0, VA, last, j, 0)
        for cs, cr, c in zc[4:]:
            recv(cr, c)
        each(nblk, unpack_f, 2)
        for j in range(C + 3):
            spread()
            if 0 <= j - 3 < C:
                k = j - 3
                d_recv(4, WB, 0, k, 4)
                lo, hi = inside(k, 5)
                residual(second, WB, 1, PV[4], lo, hi - lo, 1, put_r1)
                offer(hi)
            if 0 <= j - 2 < C:
                k = j - 2
                d_recv(3, WA, 0, k, 3)
                relax(second, WA, WB, 0, PV[3], *span(k, 4))
                d_send(4, WB, 0, k, 4)
            if 0 <= j - 1 < C:
                k = j - 1
                d_recv(1, VB, last, k, 1)
                relax(fine, VB, VC, 0, PV[1], *span(k, 2))
                d_recv(2, VC, last, k, 2)
                residual(fine, VC, nt, PV[2], *span(k, 3), 2, put_g)
                d_send(3, WA, 0, k, 3)
            if j < C:
                moved(2 * j + 1)
                for t in before:
                    relax(fine, VA, VB, t, None, *span(j, 1))
                d_send(1, VB, last, j, 1)
                d_recv(0, VA, last, j, 0)
                relax(fine, VA, VB, 0, PV[0], *span(j, 1))
                for t in before:
                    relax(fine, VB, VC, t, None, *span(j, 2))
                d_send(2, VC, last, j, 2)
        spread()

        for at in range(group // 2):
            recv(z != at, to_owner(0, at))
            recv(s < ngz - 1, strip_to(0, 0, at))
            recv(s > 0, strip_to(1, 0, at))
        turn = {"x": 0, "t": 0}

        def g_unstrip(k):
            t, b = lax.div(k, bpr), lax.rem(k, bpr)
            G[2][t, 1, pl.ds(hx[2] + b * rb, rb)] = unpack(GSr[0, k], GSr[1, k], D1)
        each(times[2] * bpr, g_unstrip, 2)

        def x_halo(at, H, depth):
            n = turn["x"]
            turn["x"] += 1
            lo = remote(at(pl.ds(H, depth)), at(pl.ds(H + xb, depth)), x_s.at[0, n], x_r.at[0, n], holder(I - 1, s))
            hi = remote(at(pl.ds(H + xb - depth, depth)), at(pl.ds(H - depth, depth)), x_s.at[1, n], x_r.at[1, n],
                        holder(I + 1, s))
            start(i > 0, lo)
            start(i < group - 1, hi)
            recv(i > 0, hi)
            recv(i < group - 1, lo)

        def t_halo(l, ver, depth, lifted=False):
            if groups == 1:
                return
            lo, n = hx[l] - depth, xb + 2 * depth
            k = turn["t"]
            turn["t"] += 1
            a, T = A[l][ver], times[l]
            rows = pl.ds(lo, n)
            to = LP[l].at[:, rows] if lifted else a.at[0, :, rows, center]
            c = remote(a.at[T, :, rows, center], to, t_s.at[k], t_r.at[k], holder(I + group, s))
            start(grp < groups - 1, c)
            recv(grp > 0, c)
            if lifted:
                @pl.when(grp > 0)
                def _():
                    for x in range(lo, lo + n):
                        for h in range(2):
                            a[0, h, x, center, :] = LP[l][h, x]

        def coarse_rows(l, lo, n, fn, steps=None):
            def step(t):
                for k in range(n):
                    fn(t, lo + k)
            each(times[l] if steps is None else steps, step)

        def first(l, depth):
            lo, n = hx[l] - depth, xb + 2 * depth

            def fn(t, x):
                for h in range(2):
                    A[l][0][t + 1, h, x, center, :] = S[l][h, x] * G[l][t, h, x]
            coarse_rows(l, lo, n, fn)
            t_halo(l, 0, depth)

        def relaxed(l, ver, depth, put):
            a = A[l][ver]
            coef = base_coef / 2.0**l

            def fn(t, x):
                c, nb = gather(a, t + 1, x, 2)
                for h in range(2):
                    b = a[t, h, x, center, :]
                    put(t, h, x, keep * c[h] + S[l][h, x] * ((G[l][t, h, x] + coef * b) + DIF[h, row0[l] + x] * nb[h]))
            coarse_rows(l, hx[l] - depth, xb + 2 * depth, fn)

        def into(l, ver):
            def put(t, h, x, val):
                A[l][ver][t + 1, h, x, center, :] = val
            return put

        def finish(l):
            def put(t, h, x, val):
                E[l][t, h, x - hx[l]] = val
            return put

        def coarse(l):
            H = hx[l]
            x_halo(lambda rows: G[l].at[:, :, rows], H, H)
            first(l, H)
            if l == LEVELS - 1:
                relaxed(l, 0, 2, into(l, 1))
                t_halo(l, 1, 2)
                relaxed(l, 1, 1, into(l, 2))
                t_halo(l, 2, 1)
                relaxed(l, 2, 0, finish(l))
                return
            relaxed(l, 0, 1, into(l, 1))
            t_halo(l, 1, 1)
            coef = base_coef / 2.0**l

            def down(t, x):
                parts = []
                d = [DIF[h, row0[l] + x] for h in range(2)]
                for k in range(2):
                    c, nb = gather(A[l][1], 2 * t + k + 1, x, 2)
                    parts.append([(G[l][2 * t + k, h, x] + coef * A[l][1][2 * t + k, h, x, center, :]) + d[h] * nb[h]
                                  - (coef + 6.0 * d[h]) * c[h] for h in range(2)])
                for h in range(2):
                    G[l + 1][t, h, x - H + hx[l + 1]] = (parts[0][h] + parts[1][h]) * 0.5
            coarse_rows(l, H, xb, down, times[l + 1])
            coarse(l + 1)

            def lift(t, x):
                for h in range(2):
                    A[l][1][t + 1, h, x, center, :] = A[l][1][t + 1, h, x, center, :] + E[l + 1][lax.div(t, 2), h, x - H]
            coarse_rows(l, H, xb, lift)
            T = times[l]
            x_halo(lambda rows: A[l][1].at[pl.ds(1, T), :, rows, center], H, 2)
            t_halo(l, 1, 2, True)
            relaxed(l, 1, 1, into(l, 2))
            t_halo(l, 2, 1)
            relaxed(l, 2, 0, finish(l))

        coarse(2)

        def drain():
            for cond, c in sends:
                @pl.when(cond)
                def _(c=c):
                    c.wait_send()
            sends.clear()
        drain()

        def e_strip(k):
            t, b = lax.div(k, bpr), lax.rem(k, bpr)
            lo, hi = pack(E[2][t, 1, pl.ds(b * rb, rb)], D0)
            ESs[k, pl.ds(0, D0)] = lo
            ESs[k, pl.ds(D0, D0)] = hi
        each(times[2] * bpr, e_strip, 2)

        def back(zz, at):
            to = holder(grp * group + 2 * zz + par, s)
            return (remote(E[2].at[zz, 0], es.at[0, pl.ds(at * xb, xb)], b_s.at[0, zz], b_r.at[0, at], to),
                    remote(ESs.at[pl.ds(zz * bpr, bpr)], ESr.at[pl.ds(at * bpr, bpr)], b_s.at[1, zz], b_r.at[1, at], to))

        for zz in range(group // 2):
            for c in back(zz, i):
                start(z != zz, c)
        for x in range(xb):
            es[0, i * xb + x] = E[2][z, 0, x]
        for b in range(bpr):
            ESr[i * bpr + b] = ESs[z * bpr + b]

        B[:] = cuts["up"]
        got = [0]

        def pass_on(o):
            rows, bl = pl.ds(o * xb, xb), pl.ds(o * bpr, bpr)
            return (remote(es.at[0, rows], es.at[0, rows], f_s.at[0, o], f_r.at[0, o], buddy),
                    remote(ESr.at[bl], ESr.at[bl], f_s.at[1, o], f_r.at[1, o], buddy))

        def arrive_up(j):
            upto = min(group, -(-B[j + 1] // xb))
            for o in range(got[0], upto):
                for c in back(0, o):
                    recv((par == o % 2) & (i != o), c)
                for c in pass_on(o):
                    start(par == o % 2, c)
            for o in range(got[0], upto):
                for c in pass_on(o):
                    recv(par != o % 2, c)
            got[0] = upto

            def fn(b):
                k = block0(j) + b
                es[1, pl.ds(k * rb, rb)] = unpack(ESr[k, pl.ds(0, D0)], ESr[k, pl.ds(D0, D0)], D0)
            each((B[j + 1] - B[j]) // rb, fn, 2)

            def lift(k):
                x = B[j] + k
                for h in range(2):
                    WB[0, h, PX + x, center, :] = WB[0, h, PX + x, center, :] + es[h, x]
            each(B[j + 1] - B[j], lift, 4)

        def lift_fine(lo, n):
            def fn(k):
                x = PX + lo + k
                e = relaxed_row(second, WA, 0, PV[6], x)
                for h in range(2):
                    for t in range(nt):
                        VC[t, h, x, center, :] = VC[t, h, x, center, :] + e[h]
            each(n, fn, 8)

        outs = []

        def emit(a, b, n):
            far = remote(a, b, o_s.at[n], o_r.at[n], flip)
            near = pltpu.make_async_copy(a, b, out_sem.at[n])
            start(swapped, far)

            @pl.when(stays)
            def _():
                near.start()
            outs.append((far, near))

        def emit_sol(j):
            lo, hi = inside(j, 4)
            emit(VB.at[:, 0, pl.ds(PX + lo, hi - lo), center], sol.at[:, pl.ds(lo, hi - lo)], j)

        def put_r(x, rs):
            for t in range(nt):
                rout[t, x] = rs[t][0]

        def emit_res(j, lo, hi):
            emit(rout.at[:, pl.ds(lo, hi - lo)], res.at[:, pl.ds(lo, hi - lo)], C + j)

        for j in range(C + 4):
            if 0 <= j - 4 < C:
                k = j - 4
                d_recv(9, VB, last, k, 4)
                lo, hi = inside(k, 5)
                residual(fine, VB, nt, PV[9], lo, hi - lo, 1, put_r)
                emit_res(k, lo, hi)
            if 0 <= j - 3 < C:
                k = j - 3
                d_recv(7, VC, last, k, 2)
                relax(fine, VC, VA, 0, PV[7], *span(k, 3))
                for t in before:
                    relax(fine, VA, VB, t, None, *span(k, 4))
                d_send(9, VB, last, k, 4)
                d_recv(8, VA, last, k, 3)
                relax(fine, VA, VB, 0, PV[8], *span(k, 4))
                emit_sol(k)
            if 0 <= j - 2 < C:
                k = j - 2
                d_recv(6, WA, 0, k, 1)
                lift_fine(*span(k, 2))
                d_send(7, VC, last, k, 2)
                for t in before:
                    relax(fine, VC, VA, t, None, *span(k, 3))
                d_send(8, VA, last, k, 3)
            if 0 <= j - 1 < C:
                k = j - 1
                d_recv(5, WB, 0, k, 0)
                relax(second, WB, WA, 0, PV[5], *span(k, 1))
                d_send(6, WA, 0, k, 1)
            if j < C:
                arrive_up(j)
                d_send(5, WB, 0, j, 0)
        for far, near in outs:
            recv(swapped, far)

            @pl.when(stays)
            def _(near=near):
                near.wait()
        drain()

    dma = pltpu.SemaphoreType.DMA
    vm = lambda *shape: pltpu.VMEM(shape, F32)
    bpr = xb // rb
    n_t = 4 * (LEVELS - 3) + 3
    n_x = 2 * (LEVELS - 3) + 1
    wide, flat = vm(nt, 2, xp, yp, nz), vm(2, xp, ny, nz)
    one = vm(1, 2, xp, yp, nz)
    scratch = [wide] * 3 + [one] * 2 + [vm(nt, 2, xp, ny, nz)] + [flat] * 4
    scratch += [vm(nt, nx, ny, nz), vm(nt, nx, ny, nz), vm(nx, ny, nz), vm(nx, ny, nz)]
    scratch += [flat] * NP
    scratch += [vm(NP, nblk + 1, 2 * D0, LANES)] * 2
    scratch += [vm(2, nt * nblk, D1, LANES)] * 2 + [vm(2, nt * nblk, D0, LANES)] * 2
    scratch += [vm(2, nblk, D1, LANES)] * 2
    scratch += [vm(2, nblk, D1, LANES), vm(2, times[2] * bpr, D1, LANES)]
    scratch += [vm(times[2] * bpr, 2 * D0, LANES), vm(nblk, 2 * D0, LANES)]
    for l in range(2, LEVELS):
        scratch += [vm(times[l] + 1, 2, xr[l], yp, nz)] * 3
    scratch += [vm(times[l], 2, xr[l], ny, nz) for l in range(2, LEVELS)]
    scratch += [vm(times[l], 2, xb, ny, nz) for l in range(2, LEVELS)]
    scratch += [vm(2, xr[l], ny, nz) for l in range(2, LEVELS)]
    scratch += [vm(2, xr[l], ny, nz) for l in range(2, LEVELS - 1)]
    scratch += [dma((3 + 2 * C + 1,)), dma((2 * C,)), dma((6,)), dma((6,)), dma((2, NP * C)), dma((2, NP * C)),
                dma((2 * C + 1,)), dma((2 * C + 1,)), dma((group,)), dma((group,)), dma((2, group)), dma((2, group)),
                dma((2, n_x)), dma((2, n_x)), dma((2, group)), dma((2, group)), dma((n_t,)), dma((n_t,)),
                dma((2 * C,)), dma((2 * C,)), dma((group,)), dma((group,)), dma((2, group)), dma((2, group))]
    shape = jax.ShapeDtypeStruct((nt, nx, ny, nz), F32)
    anyspec = pl.BlockSpec(memory_space=pl.ANY)
    return pl.pallas_call(
        kernel,
        out_shape=(shape, shape),
        in_specs=[anyspec] * 3,
        out_specs=(anyspec, anyspec),
        scratch_shapes=scratch,
        compiler_params=pltpu.CompilerParams(collective_id=0, has_side_effects=True, vmem_limit_bytes=63 << 20),
    )


def solution(mesh):
    def body(source, initial_guess, diffusivity):
        return make(mesh, *source.shape)(source, initial_guess, diffusivity)

    placed = (P("tm", None, None, "gz"), P("tm", None, None, "gz"), P(None, None, "gz"))
    return jax.shard_map(
        body,
        mesh=mesh,
        in_specs=placed,
        out_specs=(P("tm", None, None, "gz"), P("tm", None, None, "gz")),
        check_vma=False,
    )
```

```python
import jax
import jax.numpy as jnp
from jax import lax
from jax.experimental import pallas as pl
from jax.experimental.pallas import tpu as pltpu
from jax.sharding import PartitionSpec as P

LEVELS = 5
damping = 0.8
keep = 1.0 - damping
base_coef = 8.0
F32 = jnp.float32
MESH = pl.DeviceIdType.MESH
LANES = 128
PAD = 8
PX = 4
D0 = 8
D1 = 16
NP = 10
OWN_ONLY = (4, 9)


def make(mesh, nt, nx, ny, nz):
    ntm, ngz = mesh.shape["tm"], mesh.shape["gz"]
    group = 2 ** (LEVELS - 1) // nt
    groups = ntm // group
    xb = nx // group
    yp = ny + 2 * PAD
    xp = nx + 2 * PX
    rb = LANES // ny
    q = nx // 8
    cuts = {"down": [0, 2 * q, 4 * q, 6 * q, nx], "up": [0, 2 * q, 5 * q, 7 * q, nx]}
    C = len(cuts["down"]) - 1
    nblk = nx // rb
    times = [0] + [group // 2**l for l in range(LEVELS - 1)]
    hx = [0] + [2] * (LEVELS - 2) + [3]
    xr = [xb + 2 * h for h in hx]
    last = nt - 1

    def kernel(src, guess, dif_hbm, sol, res, *scr):
        scr = list(scr)
        VA, VB, VC, WA, WB, F, GL, DIF, S0, S1, HG, HF, HD, RB = [scr.pop(0) for _ in range(14)]
        rout, es, g1 = HG, HF, HD
        PV = [scr.pop(0) for _ in range(NP)]
        PSs, PSr, ZGs, ZGr, ZFs, ZFr, DSs, DSr, GSs, GSr, ESs, ESr = [scr.pop(0) for _ in range(12)]
        A = [None] * 2 + [[scr.pop(0) for _ in range(3)] for l in range(2, LEVELS)]
        G = [None] * 2 + [scr.pop(0) for _ in range(2, LEVELS)]
        E = [None] * 2 + [scr.pop(0) for _ in range(2, LEVELS)]
        S = [S0, S1] + [scr.pop(0) for _ in range(2, LEVELS)]
        LP = [None] * 2 + [scr.pop(0) for _ in range(2, LEVELS - 1)]
        (load_sem, out_sem, zs_s, zs_r, d_s, d_r, swap_s, swap_r, a_s, a_r, b_s, b_r,
         x_s, x_r, g_s, g_r, t_s, t_r, o_s, o_r, p_s, p_r, f_s, f_r) = scr

        tm, gz = lax.axis_index("tm"), lax.axis_index("gz")
        q_t, q_z = lax.rem(tm, 2), lax.rem(gz, 2)
        swapped = q_t != q_z
        stays = q_t == q_z
        I, s = tm - q_t + q_z, gz - q_z + q_t
        grp, i = lax.div(I, group), lax.rem(I, group)
        center = pl.ds(PAD, ny)
        lane = lax.broadcasted_iota(jnp.int32, (ny, nz), 1)
        m0, m1 = lane == 0, lane == nz - 1
        flip = {"tm": tm + 1 - 2 * q_t, "gz": gz + 1 - 2 * q_z}
        mate = {"tm": tm, "gz": gz + 1 - 2 * q_z}
        par, z = q_z, lax.div(i, 2)

        def holder(ii, ss):
            a, b = lax.rem(ii, 2), lax.rem(ss, 2)
            return {"tm": ii - a + b, "gz": ss - b + a}

        def remote(a, b, ss, rs, where):
            return pltpu.make_async_remote_copy(
                src_ref=a, dst_ref=b, send_sem=ss, recv_sem=rs, device_id=where, device_id_type=MESH)

        sends = []

        def start(cond, c):
            @pl.when(cond)
            def _():
                c.start()
            sends.append((cond, c))

        def recv(cond, c):
            @pl.when(cond)
            def _():
                c.wait_recv()

        def each(count, fn, unroll=1):
            whole = count // unroll

            def steps(k, _):
                for u in range(unroll):
                    fn(k * unroll + u)
                return 0
            lax.fori_loop(0, whole, steps, 0)
            for k in range(whole * unroll, count):
                fn(k)

        home = [pltpu.make_async_copy(guess, HG, load_sem.at[0]),
                pltpu.make_async_copy(src, HF, load_sem.at[1]),
                pltpu.make_async_copy(dif_hbm, HD, load_sem.at[2])]
        for c in (home[2], home[0], home[1]):
            c.start()

        zrow = jnp.zeros((ny, nz), F32)
        zpad = jnp.zeros((PAD, nz), F32)

        def clear_edges(x):
            for v in PV:
                for h in range(2):
                    v[h, x] = zrow
                    v[h, PX + nx + x] = zrow
        each(PX, clear_edges)

        bar = pltpu.get_barrier_semaphore()
        met = [jnp.int32(0)]

        def greet(cond, where):
            @pl.when(cond)
            def _():
                pl.semaphore_signal(bar, inc=1, device_id=where, device_id_type=MESH)
            met[0] = met[0] + jnp.where(cond, 1, 0)

        greet(tm >= 0, mate)
        greet(swapped, flip)
        for d in (-1, 1):
            greet((gz + d >= 0) & (gz + d < ngz), holder(tm, gz + d))
            greet((s + d >= 0) & (s + d < ngz), {"tm": I, "gz": s + d})
            greet((s + d >= 0) & (s + d < ngz), holder(I, s + d))
            greet((I + d >= 0) & (I + d < ntm), holder(I + d, s))
            if groups > 1:
                greet((grp + d >= 0) & (grp + d < groups), holder(I + d * group, s))
        for j in range(1, group):
            greet(tm >= 0, holder(grp * group + lax.rem(i + j, group), s))
            if j % 2 == 0:
                for d in (-1, 1):
                    greet((s + d >= 0) & (s + d < ngz), holder(grp * group + lax.rem(i + j, group), s + d))
        pl.semaphore_wait(bar, met[0])

        moves = {}
        for k in range(2):
            for j in range(C):
                first, many = cuts["down"][j], cuts["down"][j + 1] - cuts["down"][j]
                rows, there = pl.ds(first, many), pl.ds(PX + first, many)
                h, v = ((guess.at[:, rows], VA.at[:, 0, there, center]) if k == 0 else
                        (src.at[:, rows], F.at[:, 0, there]))
                n = 2 * j + k
                far = remote(h, v, swap_s.at[n], swap_r.at[n], flip)
                near = pltpu.make_async_copy(h, v, load_sem.at[3 + n])
                start(swapped, far)

                @pl.when(stays)
                def _(near=near):
                    near.start()
                moves[n] = (far, near)
        dif_own = pltpu.make_async_copy(dif_hbm, DIF.at[0, pl.ds(PX, nx)], load_sem.at[3 + 2 * C])
        dif_far = remote(dif_hbm, DIF.at[0, pl.ds(PX, nx)], swap_s.at[2 * C], swap_r.at[2 * C], mate)
        start(stays, dif_far)

        @pl.when(stays)
        def _():
            dif_own.start()

        def moved(n):
            far, near = moves[n]
            recv(swapped, far)

            @pl.when(stays)
            def _():
                near.wait()

        def clear_v(x):
            for v in (VA, VB, VC):
                for t in range(nt):
                    for h in range(2):
                        v[t, h, x, pl.ds(0, PAD), :] = zpad
                        v[t, h, x, pl.ds(PAD + ny, PAD), :] = zpad
            for v in (WA, WB):
                for h in range(2):
                    v[0, h, x, pl.ds(0, PAD), :] = zpad
                    v[0, h, x, pl.ds(PAD + ny, PAD), :] = zpad
        each(xp, clear_v)

        def clear_x(x):
            for xx in (x, PX + nx + x):
                for h in range(2):
                    for t in range(nt):
                        for v in (VA, VB, VC):
                            v[t, h, xx, center, :] = zrow
                        F[t, h, xx] = zrow
                    for v in (WA, WB):
                        v[0, h, xx, center, :] = zrow
                    DIF[h, xx] = zrow
                    GL[h, xx] = zrow
        each(PX, clear_x)

        @pl.when(I == 0)
        def _():
            def clear_p(x):
                for v in PV:
                    for h in range(2):
                        v[h, PX + x] = zrow
            each(nx, clear_p)
        for l in range(2, LEVELS):
            def clear_a(t, l=l):
                for h in range(2):
                    for a in A[l]:
                        for x in range(xr[l]):
                            a[t + 1, h, x, pl.ds(0, PAD), :] = zpad
                            a[t + 1, h, x, pl.ds(PAD + ny, PAD), :] = zpad
                    for x in range(hx[l]):
                        for xx in (x, hx[l] + xb + x):
                            G[l][t, h, xx] = zrow
                            A[l][1][t + 1, h, xx, center, :] = zrow
            each(times[l], clear_a)

            @pl.when(grp == 0)
            def _(l=l):
                def clear_b(x):
                    for h in range(2):
                        for a in A[l]:
                            a[0, h, x, center, :] = zrow
                each(xr[l], clear_b)

        def pack(block, depth):
            tr = block.reshape(rb * ny, nz).T
            return tr[:depth], tr[nz - depth:]

        def unpack(lo, hi, depth):
            mid = jnp.zeros((nz - 2 * depth, LANES), F32)
            return jnp.concatenate([lo, mid, hi], axis=0).T.reshape(rb, ny, nz)

        for side, edge in ((0, s == ngz - 1), (1, s == 0)):
            @pl.when(edge)
            def _(side=side):
                for a in (ZGr, ZFr, DSr, GSr):
                    def clear_z(k, a=a):
                        a[side, k] = jnp.zeros(a.shape[2:], F32)
                    each(a.shape[1], clear_z)

        home[2].wait()

        def pack_d(b):
            lo, hi = pack(HD[pl.ds(b * rb, rb)], D1)
            DSs[0, b] = lo
            DSs[1, b] = hi
        each(nblk, pack_d, 2)
        home[0].wait()
        home[1].wait()

        def pack_h(b):
            for h, a, depth in ((HG, ZGs, D1), (HF, ZFs, D0)):
                for t in range(nt):
                    lo, hi = pack(h[t, pl.ds(b * rb, rb)], depth)
                    a[0, t * nblk + b] = lo
                    a[1, t * nblk + b] = hi
        each(nblk, pack_h)

        def z_pair(side, a, b, n, home_side):
            d = -1 if side == 0 else 1
            to = holder(tm, gz + d) if home_side else holder(I, s + d)
            c = remote(a.at[side], b.at[side], zs_s.at[n], zs_r.at[n], to)
            base = gz if home_side else s
            can_send = (base + d >= 0) & (base + d < ngz)
            can_recv = (s - d >= 0) & (s - d < ngz)
            return can_send, can_recv, c

        zc = [z_pair(side, a, b, 2 * k + side, True) for k, (a, b) in enumerate(((DSs, DSr), (ZGs, ZGr), (ZFs, ZFr))) for side in range(2)]
        for cs, cr, c in zc:
            start(cs, c)

        @pl.when(stays)
        def _():
            dif_own.wait()
        recv(swapped, dif_far)
        for cs, cr, c in zc[:2]:
            recv(cr, c)

        def unpack_d(b):
            DIF[1, pl.ds(PX + b * rb, rb)] = unpack(DSr[0, b], DSr[1, b], D1)
        each(nblk, unpack_d, 2)

        def scales(x):
            for h in range(2):
                S0[h, x] = damping / (base_coef + 6.0 * DIF[h, x])
                S1[h, x] = damping / (base_coef / 2.0 + 6.0 * DIF[h, x])
        each(xp, scales)
        row0 = [i * xb + PX - h for h in hx]
        for l in range(2, LEVELS):
            def scales_l(x, l=l):
                for h in range(2):
                    S[l][h, x] = damping / (base_coef / 2.0**l + 6.0 * DIF[h, row0[l] + x])
            each(xr[l], scales_l)
        for cs, cr, c in zc[2:4]:
            recv(cr, c)

        def unpack_g(b):
            for t in range(nt):
                VA[t, 1, pl.ds(PX + b * rb, rb), center, :] = unpack(ZGr[0, t * nblk + b], ZGr[1, t * nblk + b], D1)
        each(nblk, unpack_g, 2)

        def unpack_f(b):
            for t in range(nt):
                F[t, 1, pl.ds(PX + b * rb, rb)] = unpack(ZFr[0, t * nblk + b], ZFr[1, t * nblk + b], D0)

        def gather(v, t, x, parts):
            c = [v[t, h, x, center, :] for h in range(2)]
            up = [pltpu.roll(a, 1, 1) for a in c]
            dn = [pltpu.roll(a, nz - 1, 1) for a in c]
            nb = []
            for h in range(parts):
                a = v[t, h, x + 1, center, :] + v[t, h, x - 1, center, :]
                a = a + (v[t, h, x, pl.ds(PAD + 1, ny), :] + v[t, h, x, pl.ds(PAD - 1, ny), :])
                nb.append(a + (jnp.where(m0, up[1 - h], up[h]) + jnp.where(m1, dn[1 - h], dn[h])))
            return c, nb

        fine = (lambda t, h, x: F[t, h, x], S0, base_coef)
        second = (lambda t, h, x: GL[h, x], S1, base_coef / 2.0)

        def relaxed_row(lev, v, t, pv, x):
            g, sc, coef = lev
            c, nb = gather(v, t, x, 2)
            b = [pv[h, x] if t == 0 else v[t - 1, h, x, center, :] for h in range(2)]
            return [keep * c[h] + sc[h, x] * ((g(t, h, x) + coef * b[h]) + DIF[h, x] * nb[h]) for h in range(2)]

        def relax(lev, v, w, t, pv, lo, n):
            def fn(k):
                x = PX + lo + k
                val = relaxed_row(lev, v, t, pv, x)
                for h in range(2):
                    w[t, h, x, center, :] = val[h]
            each(n, fn, 8)

        def residual(lev, v, steps, pv, lo, n, parts, put):
            g, _, coef = lev

            def fn(k):
                x = PX + lo + k
                d = [DIF[h, x] for h in range(parts)]
                b = [pv[h, x] for h in range(parts)]
                rs = []
                for t in range(steps):
                    c, nb = gather(v, t, x, parts)
                    rs.append([(g(t, h, x) + coef * b[h]) + d[h] * nb[h] - (coef + 6.0 * d[h]) * c[h] for h in range(parts)])
                    b = c
                put(lo + k, rs)
            each(n, fn, 4 if parts * steps > 2 else 8)

        B = list(cuts["down"])

        def span(j, off):
            hi = B[j + 1] - off if j < C - 1 else nx
            if j == 0:
                m = -(-hi // rb) * rb
                return hi - m, m
            return B[j] - off, -(-(hi - B[j] + off) // rb) * rb

        def block0(j):
            return B[j] // rb

        def inside(j, off):
            return max(B[j] - off, 0), (B[j + 1] - off if j < C - 1 else nx)

        def d_copies(n, v, t, j, off):
            lo, m = span(j, off)
            rows = pl.ds(PX + lo, m)
            k = n * C + j
            bl = pl.ds(block0(j), m // rb)
            own = remote(v.at[t, 0, rows, center], PV[n].at[0, rows], d_s.at[0, k], d_r.at[0, k], holder(I + 1, s))
            halo = remote(PSs.at[n, bl], PSr.at[n, bl], d_s.at[1, k], d_r.at[1, k], holder(I + 1, s))
            return own, halo

        def d_send(n, v, t, j, off):
            lo, m = span(j, off)

            def fn(b):
                lo8, hi8 = pack(v[t, 1, pl.ds(PX + lo + b * rb, rb), center, :], D0)
                PSs[n, block0(j) + b, pl.ds(0, D0)] = lo8
                PSs[n, block0(j) + b, pl.ds(D0, D0)] = hi8
            own, halo = d_copies(n, v, t, j, off)
            start(I < ntm - 1, own)
            if n not in OWN_ONLY:
                each(m // rb, fn, 3)
                start(I < ntm - 1, halo)

        def d_recv(n, v, t, j, off):
            lo, m = span(j, off)
            own, halo = d_copies(n, v, t, j, off)

            @pl.when(I > 0)
            def _():
                own.wait_recv()
                if n in OWN_ONLY:
                    return
                halo.wait_recv()

                def fn(b):
                    k = block0(j) + b
                    PV[n][1, pl.ds(PX + lo + b * rb, rb)] = unpack(PSr[n, k, pl.ds(0, D0)], PSr[n, k, pl.ds(D0, D0)], D0)
                each(m // rb, fn, 3)

        before = range(nt - 1, 0, -1)

        def put_g(x, rs):
            for h in range(2):
                g = (rs[0][h] + rs[1][h]) * 0.5
                GL[h, PX + x] = g
                WA[0, h, PX + x, center, :] = S1[h, PX + x] * g

        def put_r1(x, rs):
            g1[x] = rs[0][0]

        bpr = xb // rb
        buddy = holder(I + 1 - 2 * par, s)

        def to_buddy(o):
            rows = pl.ds(o * xb, xb)
            return remote(g1.at[rows], RB.at[rows], p_s.at[o], p_r.at[o], buddy)

        def to_owner(o, at):
            return remote(g1.at[pl.ds(o * xb, xb)], G[2].at[at, 0, pl.ds(hx[2], xb)], a_s.at[o], a_r.at[at],
                          holder(grp * group + o, s))

        def strip_to(side, o, at):
            d = -1 if side == 0 else 1
            return remote(GSs.at[side, pl.ds(o * bpr, bpr)], GSr.at[side, pl.ds(at * bpr, bpr)], g_s.at[side, o],
                          g_r.at[side, at], holder(grp * group + o, s + d))

        ready, sent = [0], [0]

        def offer(hi):
            while ready[0] < group and (ready[0] + 1) * xb <= hi:
                start(par != ready[0] % 2, to_buddy(ready[0]))
                ready[0] += 1

        def spread():
            while sent[0] < ready[0]:
                o = sent[0]
                sent[0] += 1
                mine = par == o % 2
                recv(mine, to_buddy(o))

                @pl.when(mine)
                def _(o=o):
                    def fn(b):
                        rows = pl.ds(o * xb + b * rb, rb)
                        g = (g1[rows] + RB[rows]) * 0.5
                        g1[rows] = g
                        lo, hi = pack(g, D1)
                        GSs[0, o * bpr + b] = lo
                        GSs[1, o * bpr + b] = hi
                    each(bpr, fn)
                start(mine & (i != o), to_owner(o, z))
                start(mine & (s > 0), strip_to(0, o, z))
                start(mine & (s < ngz - 1), strip_to(1, o, z))

                @pl.when(i == o)
                def _(o=o):
                    for x in range(xb):
                        G[2][z, 0, hx[2] + x] = g1[o * xb + x]

        for j in range(C):
            moved(2 * j)
            d_send(0, VA, last, j, 0)
        for cs, cr, c in zc[4:]:
            recv(cr, c)
        each(nblk, unpack_f, 2)
        for j in range(C + 3):
            spread()
            if 0 <= j - 3 < C:
                k = j - 3
                d_recv(4, WB, 0, k, 4)
                lo, hi = inside(k, 5)
                residual(second, WB, 1, PV[4], lo, hi - lo, 1, put_r1)
                offer(hi)
            if 0 <= j - 2 < C:
                k = j - 2
                d_recv(3, WA, 0, k, 3)
                relax(second, WA, WB, 0, PV[3], *span(k, 4))
                d_send(4, WB, 0, k, 4)
            if 0 <= j - 1 < C:
                k = j - 1
                d_recv(1, VB, last, k, 1)
                relax(fine, VB, VC, 0, PV[1], *span(k, 2))
                d_recv(2, VC, last, k, 2)
                residual(fine, VC, nt, PV[2], *span(k, 3), 2, put_g)
                d_send(3, WA, 0, k, 3)
            if j < C:
                moved(2 * j + 1)
                for t in before:
                    relax(fine, VA, VB, t, None, *span(j, 1))
                d_send(1, VB, last, j, 1)
                d_recv(0, VA, last, j, 0)
                relax(fine, VA, VB, 0, PV[0], *span(j, 1))
                for t in before:
                    relax(fine, VB, VC, t, None, *span(j, 2))
                d_send(2, VC, last, j, 2)
        spread()

        for at in range(group // 2):
            recv(z != at, to_owner(0, at))
            recv(s < ngz - 1, strip_to(0, 0, at))
            recv(s > 0, strip_to(1, 0, at))
        turn = {"x": 0, "t": 0}

        def g_unstrip(k):
            t, b = lax.div(k, bpr), lax.rem(k, bpr)
            G[2][t, 1, pl.ds(hx[2] + b * rb, rb)] = unpack(GSr[0, k], GSr[1, k], D1)
        each(times[2] * bpr, g_unstrip, 2)

        def x_halo(at, H, depth):
            n = turn["x"]
            turn["x"] += 1
            lo = remote(at(pl.ds(H, depth)), at(pl.ds(H + xb, depth)), x_s.at[0, n], x_r.at[0, n], holder(I - 1, s))
            hi = remote(at(pl.ds(H + xb - depth, depth)), at(pl.ds(H - depth, depth)), x_s.at[1, n], x_r.at[1, n],
                        holder(I + 1, s))
            start(i > 0, lo)
            start(i < group - 1, hi)
            recv(i > 0, hi)
            recv(i < group - 1, lo)

        def t_halo(l, ver, depth, lifted=False):
            if groups == 1:
                return
            lo, n = hx[l] - depth, xb + 2 * depth
            k = turn["t"]
            turn["t"] += 1
            a, T = A[l][ver], times[l]
            rows = pl.ds(lo, n)
            to = LP[l].at[:, rows] if lifted else a.at[0, :, rows, center]
            c = remote(a.at[T, :, rows, center], to, t_s.at[k], t_r.at[k], holder(I + group, s))
            start(grp < groups - 1, c)
            recv(grp > 0, c)
            if lifted:
                @pl.when(grp > 0)
                def _():
                    for x in range(lo, lo + n):
                        for h in range(2):
                            a[0, h, x, center, :] = LP[l][h, x]

        def coarse_rows(l, lo, n, fn, steps=None):
            def step(t):
                for k in range(n):
                    fn(t, lo + k)
            each(times[l] if steps is None else steps, step)

        def first(l, depth):
            lo, n = hx[l] - depth, xb + 2 * depth

            def fn(t, x):
                for h in range(2):
                    A[l][0][t + 1, h, x, center, :] = S[l][h, x] * G[l][t, h, x]
            coarse_rows(l, lo, n, fn)
            t_halo(l, 0, depth)

        def relaxed(l, ver, depth, put):
            a = A[l][ver]
            coef = base_coef / 2.0**l

            def fn(t, x):
                c, nb = gather(a, t + 1, x, 2)
                for h in range(2):
                    b = a[t, h, x, center, :]
                    put(t, h, x, keep * c[h] + S[l][h, x] * ((G[l][t, h, x] + coef * b) + DIF[h, row0[l] + x] * nb[h]))
            coarse_rows(l, hx[l] - depth, xb + 2 * depth, fn)

        def into(l, ver):
            def put(t, h, x, val):
                A[l][ver][t + 1, h, x, center, :] = val
            return put

        def finish(l):
            def put(t, h, x, val):
                E[l][t, h, x - hx[l]] = val
            return put

        def coarse(l):
            H = hx[l]
            x_halo(lambda rows: G[l].at[:, :, rows], H, H)
            first(l, H)
            if l == LEVELS - 1:
                relaxed(l, 0, 2, into(l, 1))
                t_halo(l, 1, 2)
                relaxed(l, 1, 1, into(l, 2))
                t_halo(l, 2, 1)
                relaxed(l, 2, 0, finish(l))
                return
            relaxed(l, 0, 1, into(l, 1))
            t_halo(l, 1, 1)
            coef = base_coef / 2.0**l

            def down(t, x):
                parts = []
                d = [DIF[h, row0[l] + x] for h in range(2)]
                for k in range(2):
                    c, nb = gather(A[l][1], 2 * t + k + 1, x, 2)
                    parts.append([(G[l][2 * t + k, h, x] + coef * A[l][1][2 * t + k, h, x, center, :]) + d[h] * nb[h]
                                  - (coef + 6.0 * d[h]) * c[h] for h in range(2)])
                for h in range(2):
                    G[l + 1][t, h, x - H + hx[l + 1]] = (parts[0][h] + parts[1][h]) * 0.5
            coarse_rows(l, H, xb, down, times[l + 1])
            coarse(l + 1)

            def lift(t, x):
                for h in range(2):
                    A[l][1][t + 1, h, x, center, :] = A[l][1][t + 1, h, x, center, :] + E[l + 1][lax.div(t, 2), h, x - H]
            coarse_rows(l, H, xb, lift)
            T = times[l]
            x_halo(lambda rows: A[l][1].at[pl.ds(1, T), :, rows, center], H, 2)
            t_halo(l, 1, 2, True)
            relaxed(l, 1, 1, into(l, 2))
            t_halo(l, 2, 1)
            relaxed(l, 2, 0, finish(l))

        coarse(2)

        def drain():
            for cond, c in sends:
                @pl.when(cond)
                def _(c=c):
                    c.wait_send()
            sends.clear()
        drain()

        def e_strip(k):
            t, b = lax.div(k, bpr), lax.rem(k, bpr)
            lo, hi = pack(E[2][t, 1, pl.ds(b * rb, rb)], D0)
            ESs[k, pl.ds(0, D0)] = lo
            ESs[k, pl.ds(D0, D0)] = hi
        each(times[2] * bpr, e_strip, 2)

        def back(zz, at):
            to = holder(grp * group + 2 * zz + par, s)
            return (remote(E[2].at[zz, 0], es.at[0, pl.ds(at * xb, xb)], b_s.at[0, zz], b_r.at[0, at], to),
                    remote(ESs.at[pl.ds(zz * bpr, bpr)], ESr.at[pl.ds(at * bpr, bpr)], b_s.at[1, zz], b_r.at[1, at], to))

        for zz in range(group // 2):
            for c in back(zz, i):
                start(z != zz, c)
        for x in range(xb):
            es[0, i * xb + x] = E[2][z, 0, x]
        for b in range(bpr):
            ESr[i * bpr + b] = ESs[z * bpr + b]

        B[:] = cuts["up"]
        got = [0]

        def pass_on(o):
            rows, bl = pl.ds(o * xb, xb), pl.ds(o * bpr, bpr)
            return (remote(es.at[0, rows], es.at[0, rows], f_s.at[0, o], f_r.at[0, o], buddy),
                    remote(ESr.at[bl], ESr.at[bl], f_s.at[1, o], f_r.at[1, o], buddy))

        def arrive_up(j):
            upto = min(group, -(-B[j + 1] // xb))
            for o in range(got[0], upto):
                for c in back(0, o):
                    recv((par == o % 2) & (i != o), c)
                for c in pass_on(o):
                    start(par == o % 2, c)
            for o in range(got[0], upto):
                for c in pass_on(o):
                    recv(par != o % 2, c)
            got[0] = upto

            def fn(b):
                k = block0(j) + b
                es[1, pl.ds(k * rb, rb)] = unpack(ESr[k, pl.ds(0, D0)], ESr[k, pl.ds(D0, D0)], D0)
            each((B[j + 1] - B[j]) // rb, fn, 2)

            def lift(k):
                x = B[j] + k
                for h in range(2):
                    WB[0, h, PX + x, center, :] = WB[0, h, PX + x, center, :] + es[h, x]
            each(B[j + 1] - B[j], lift, 4)

        def lift_fine(lo, n):
            def fn(k):
                x = PX + lo + k
                e = relaxed_row(second, WA, 0, PV[6], x)
                for h in range(2):
                    for t in range(nt):
                        VC[t, h, x, center, :] = VC[t, h, x, center, :] + e[h]
            each(n, fn, 8)

        outs = []

        def emit(a, b, n):
            far = remote(a, b, o_s.at[n], o_r.at[n], flip)
            near = pltpu.make_async_copy(a, b, out_sem.at[n])
            start(swapped, far)

            @pl.when(stays)
            def _():
                near.start()
            outs.append((far, near))

        def emit_sol(j, t):
            lo, hi = inside(j, 4)
            emit(VB.at[t, 0, pl.ds(PX + lo, hi - lo), center], sol.at[t, pl.ds(lo, hi - lo)], t * C + j)

        def put_r(x, rs):
            for t in range(nt):
                rout[t, x] = rs[t][0]

        def emit_res(j, lo, hi):
            emit(rout.at[:, pl.ds(lo, hi - lo)], res.at[:, pl.ds(lo, hi - lo)], nt * C + j)

        for j in range(C + 4):
            if 0 <= j - 4 < C:
                k = j - 4
                d_recv(9, VB, last, k, 4)
                lo, hi = inside(k, 5)
                residual(fine, VB, nt, PV[9], lo, hi - lo, 1, put_r)
                emit_res(k, lo, hi)
            if 0 <= j - 3 < C:
                k = j - 3
                d_recv(7, VC, last, k, 2)
                relax(fine, VC, VA, 0, PV[7], *span(k, 3))
                for t in before:
                    relax(fine, VA, VB, t, None, *span(k, 4))
                    emit_sol(k, t)
                d_send(9, VB, last, k, 4)
                d_recv(8, VA, last, k, 3)
                relax(fine, VA, VB, 0, PV[8], *span(k, 4))
                emit_sol(k, 0)
            if 0 <= j - 2 < C:
                k = j - 2
                d_recv(6, WA, 0, k, 1)
                lift_fine(*span(k, 2))
                d_send(7, VC, last, k, 2)
                for t in before:
                    relax(fine, VC, VA, t, None, *span(k, 3))
                d_send(8, VA, last, k, 3)
            if 0 <= j - 1 < C:
                k = j - 1
                d_recv(5, WB, 0, k, 0)
                relax(second, WB, WA, 0, PV[5], *span(k, 1))
                d_send(6, WA, 0, k, 1)
            if j < C:
                arrive_up(j)
                d_send(5, WB, 0, j, 0)
        for far, near in outs:
            recv(swapped, far)

            @pl.when(stays)
            def _(near=near):
                near.wait()
        drain()

    dma = pltpu.SemaphoreType.DMA
    vm = lambda *shape: pltpu.VMEM(shape, F32)
    bpr = xb // rb
    n_t = 4 * (LEVELS - 3) + 3
    n_x = 2 * (LEVELS - 3) + 1
    wide, flat = vm(nt, 2, xp, yp, nz), vm(2, xp, ny, nz)
    one = vm(1, 2, xp, yp, nz)
    scratch = [wide] * 3 + [one] * 2 + [vm(nt, 2, xp, ny, nz)] + [flat] * 4
    scratch += [vm(nt, nx, ny, nz), vm(nt, nx, ny, nz), vm(nx, ny, nz), vm(nx, ny, nz)]
    scratch += [flat] * NP
    scratch += [vm(NP, nblk + 1, 2 * D0, LANES)] * 2
    scratch += [vm(2, nt * nblk, D1, LANES)] * 2 + [vm(2, nt * nblk, D0, LANES)] * 2
    scratch += [vm(2, nblk, D1, LANES)] * 2
    scratch += [vm(2, nblk, D1, LANES), vm(2, times[2] * bpr, D1, LANES)]
    scratch += [vm(times[2] * bpr, 2 * D0, LANES), vm(nblk, 2 * D0, LANES)]
    for l in range(2, LEVELS):
        scratch += [vm(times[l] + 1, 2, xr[l], yp, nz)] * 3
    scratch += [vm(times[l], 2, xr[l], ny, nz) for l in range(2, LEVELS)]
    scratch += [vm(times[l], 2, xb, ny, nz) for l in range(2, LEVELS)]
    scratch += [vm(2, xr[l], ny, nz) for l in range(2, LEVELS)]
    scratch += [vm(2, xr[l], ny, nz) for l in range(2, LEVELS - 1)]
    scratch += [dma((3 + 2 * C + 1,)), dma(((nt + 1) * C,)), dma((6,)), dma((6,)), dma((2, NP * C)), dma((2, NP * C)),
                dma((2 * C + 1,)), dma((2 * C + 1,)), dma((group,)), dma((group,)), dma((2, group)), dma((2, group)),
                dma((2, n_x)), dma((2, n_x)), dma((2, group)), dma((2, group)), dma((n_t,)), dma((n_t,)),
                dma(((nt + 1) * C,)), dma(((nt + 1) * C,)), dma((group,)), dma((group,)), dma((2, group)), dma((2, group))]
    shape = jax.ShapeDtypeStruct((nt, nx, ny, nz), F32)
    anyspec = pl.BlockSpec(memory_space=pl.ANY)
    return pl.pallas_call(
        kernel,
        out_shape=(shape, shape),
        in_specs=[anyspec] * 3,
        out_specs=(anyspec, anyspec),
        scratch_shapes=scratch,
        compiler_params=pltpu.CompilerParams(collective_id=0, has_side_effects=True, vmem_limit_bytes=63 << 20),
    )


def solution(mesh):
    def body(source, initial_guess, diffusivity):
        return make(mesh, *source.shape)(source, initial_guess, diffusivity)

    placed = (P("tm", None, None, "gz"), P("tm", None, None, "gz"), P(None, None, "gz"))
    return jax.shard_map(
        body,
        mesh=mesh,
        in_specs=placed,
        out_specs=(P("tm", None, None, "gz"), P("tm", None, None, "gz")),
        check_vma=False,
    )
```
